32 devices in a mesh: outer: 4 (over y, core), inner: 8 (over z, x).
Axes of the slice: x: 2, y: 2, z: 4, core: 2. Of those that a mesh axis runs over, the one named last changes fastest.
Arguments:
- tokens: bfloat16 [12288, 4096], P(('outer', 'inner')), may hold values from -6 to 6
- out_grad: bfloat16 [12288, 1024], P(('outer', 'inner')), may hold values from -0.3125 to 0.3125
- master_weights: float32 [1024, 4096], P(('outer', 'inner')), may hold values from -0.0421 to 0.0421
- base_weights: bfloat16 [1024, 4096], replicated, may hold values from -0.030029297 to 0.030029297
- adam_m: float32 [1024, 4096], P(('outer', 'inner')), may hold values from -8 to 8
- adam_v: float32 [1024, 4096], P(('outer', 'inner')), may hold values from 0.1 to 10
- grad_exps: int32 [32, 8, 32], P(('outer', 'inner')), may hold values from -13 to -8
- diff_exps: int32 [1024, 32], P(('outer', 'inner')), may hold values from -20 to -15
- hadamard_signs: int32 [32, 128], replicated, may hold values 0 or 1
Outputs:
- projected: bfloat16 [12288, 1024], P(('outer', 'inner'))
- new_master: float32 [1024, 4096], P(('outer', 'inner'))
- new_first: float32 [1024, 4096], P(('outer', 'inner'))
- new_second: float32 [1024, 4096], P(('outer', 'inner'))
The draws below stay inside these ranges and needn't reach their ends.
All inputs are finite; a program needn't handle non-finite values.
Results may differ from the reference program's by a relative error of at most 0.005.
Values may be sent and summed in bfloat16 or wider, within the bound.
A program may use at most 128 MiB of HBM per device.

```python
import math
import jax
import jax.numpy as jnp
from jax import lax

D = 4096
KV = 1024
HB = 128
ADAM_STEP = 10
TOK_DEV = 384
BLOCKS = 32
TOKENS = 12288


def shared_weights(key):
    base_key = jax.random.fold_in(key, 11)
    drift_key = jax.random.fold_in(key, 23)
    base_rows = jax.random.uniform(base_key, (KV, D), jnp.float32, -0.03, 0.03)
    drift_rows = jax.random.truncated_normal(drift_key, -4.0, 4.0, (KV, D), jnp.float32) * 0.003
    base_half = base_rows.astype(jnp.bfloat16)
    return (base_half, base_half.astype(jnp.float32) + drift_rows)


def draw_base_weights(key, part):
    return shared_weights(key)[0]


def draw_master_weights(key, part):
    return shared_weights(key)[1]


def with_ends(array, own_key, smallest, top_value):
    longest = array.shape.index(max(array.shape))
    spots = []
    for shift in (0, 1):
        where = [jax.random.randint(jax.random.fold_in(own_key, axis), (), 0, length) for axis, length in enumerate(array.shape)]
        where[longest] = (where[longest] + shift) % array.shape[longest]
        spots.append(tuple(where))
    return array.at[spots[0]].set(smallest).at[spots[1]].set(top_value)


def raised(result, key, source, target, shards_of, factor):
    def block_of(dim):
        return (jnp.arange(result.shape[dim]) // (result.shape[dim] // shards_of)).reshape((-1,) + (1,) * (result.ndim - 1 - dim))

    one_side = jax.random.permutation(key, shards_of)[block_of(target)]
    far = (block_of(target) + shards_of // 2) % shards_of
    return jnp.where((block_of(source) == one_side) | (block_of(source) == far), factor * result, result)


def levels(own_key, dims, cuts, smallest, high):
    level = 1.0
    for axis_at, blocks in cuts:
        draws = jax.random.uniform(jax.random.fold_in(jax.random.fold_in(own_key, 6), axis_at), (blocks,), jnp.float32, smallest / len(cuts), high / len(cuts))
        level = level * jnp.repeat(jnp.exp(draws), dims[axis_at] // blocks).reshape((-1,) + (1,) * (len(dims) - 1 - axis_at))
    return level


def gaussian(stream_key, shape, scale, reach, shards=(), held_as=jnp.bfloat16):
    factor_of = levels(stream_key, shape, shards, -0.22, 0.18) if shards else 1.0
    drawn = jax.random.normal(stream_key, shape, jnp.float32) * scale * factor_of
    return jnp.minimum(jnp.maximum(drawn, -reach), reach).astype(held_as)


def gaussian_with(own_key, dims, spread, limit, cuts, heavy, kind=jnp.bfloat16):
    array = spread * jax.random.normal(own_key, dims, jnp.float32)
    if cuts:
        array = array * levels(own_key, dims, cuts, -0.22, 0.18)
    return jnp.clip(raised(array, jax.random.fold_in(own_key, 3), *heavy), -limit, limit).astype(kind)


def setup_inputs(seed: int = 0) -> dict:
    seeds = jax.random.split(jax.random.key(seed), 10)
    tokens = gaussian(seeds[0], (TOKENS, D), 1.0, 6.0, ((0, 32),))
    out_grad = gaussian_with(seeds[1], (TOKENS, KV), (TOKENS // 9) ** -0.5, 0.3125, ((0, 32),), (0, 1, 32, 2.75))
    master_weights = draw_master_weights(jax.random.fold_in(seeds[9], 71), 0)
    base_weights = draw_base_weights(jax.random.fold_in(seeds[9], 71), 0)
    adam_m = gaussian(seeds[4], (KV, D), 2.0, 8.0, ((0, 32),), jnp.float32)
    adam_v = jnp.clip(jnp.exp(math.log(10.0) - 4.6051702 * jax.random.uniform(seeds[5], (KV, D), jnp.float32) ** levels(seeds[5], (KV, D), ((0, 32),), -0.2, 0.2)), 0.1, 10.0)
    grad_exps = with_ends(jax.random.randint(seeds[6], (BLOCKS, KV // HB, D // HB), -13, -7), jax.random.fold_in(seeds[6], 1), -13, (-7) - 1).astype(jnp.int32)
    diff_exps = with_ends(jax.random.randint(seeds[7], (KV, D // HB), -20, -14), jax.random.fold_in(seeds[7], 1), -20, (-14) - 1).astype(jnp.int32)
    hadamard_signs = with_ends((jax.random.randint(seeds[8], (D // HB, HB), 0, 2) < 1).astype(jnp.int32), jax.random.fold_in(seeds[8], 1), 0, 1)
    return {"tokens": tokens, "out_grad": out_grad, "master_weights": master_weights, "base_weights": base_weights, "adam_m": adam_m, "adam_v": adam_v, "grad_exps": grad_exps, "diff_exps": diff_exps, "hadamard_signs": hadamard_signs}


clip_level = 448.0
beta_one = 0.9
beta_two = 0.95
learn_rate = 0.002
decay_rate = 0.1
adam_eps = 1e-08
highest = lax.Precision.HIGHEST

def hadamard(matrix_size):
    positions = jnp.arange(matrix_size, dtype=jnp.int32)
    common = positions[:, None] & positions[None, :]
    parity = jnp.zeros((matrix_size, matrix_size), jnp.int32)
    for bit_level in range(matrix_size.bit_length() - 1):
        parity = parity + (common >> bit_level & 1)
    return (1 - 2 * (parity % 2)).astype(jnp.float32)

def rotate_rows(row_block, sign_rows, matrix):
    row_count = row_block.shape[0]
    blocks = row_block.reshape(row_count, sign_rows.shape[0], sign_rows.shape[1]) * sign_rows
    turned = jnp.dot(blocks.reshape(-1, sign_rows.shape[1]), matrix, precision=highest)
    return turned.reshape(row_block.shape) / math.sqrt(sign_rows.shape[1])

def unrotate_rows(row_block, sign_rows, matrix):
    row_count = row_block.shape[0]
    turned = jnp.dot(row_block.reshape(-1, sign_rows.shape[1]), matrix, precision=highest) / math.sqrt(sign_rows.shape[1])
    return (turned.reshape(row_count, sign_rows.shape[0], sign_rows.shape[1]) * sign_rows).reshape(row_block.shape)

def clip_rows(row_block, bound_rows):
    row_count = row_block.shape[0]
    shaped = row_block.reshape(row_count, bound_rows.shape[1], -1)
    limits = bound_rows[:, :, None]
    return jnp.clip(shaped, -limits, limits).reshape(row_block.shape)

def adam_update(gradient, master, first, second):
    new_first = beta_one * first + (1.0 - beta_one) * gradient
    new_second = beta_two * second + (1.0 - beta_two) * gradient * gradient
    fix_one = 1.0 - beta_one ** ADAM_STEP
    fix_two = 1.0 - beta_two ** ADAM_STEP
    step_dir = new_first / fix_one / (jnp.sqrt(new_second / fix_two) + adam_eps)
    new_master = master - learn_rate * (step_dir + decay_rate * master)
    return (new_master, new_first, new_second)

def reference(tokens, out_grad, master_weights, base_weights, adam_m, adam_v, grad_exps, diff_exps, hadamard_signs):
    sign_rows = (2 * hadamard_signs - 1).astype(jnp.float32)
    matrix = hadamard(HB)

    def add_block(total, block_id):
        rows_x = lax.dynamic_slice_in_dim(tokens, block_id * TOK_DEV, TOK_DEV, 0)
        rows_g = lax.dynamic_slice_in_dim(out_grad, block_id * TOK_DEV, TOK_DEV, 0)
        term_rows = lax.dot_general(rows_g, rows_x, (((0,), (0,)), ((), ())), preferred_element_type=jnp.float32)
        turned = rotate_rows(term_rows, sign_rows, matrix)
        exps_here = lax.dynamic_index_in_dim(grad_exps, block_id, 0, keepdims=False)
        bound_rows = jnp.repeat(clip_level * jnp.exp2(exps_here.astype(jnp.float32)), HB, axis=0)
        coded_rows = lax.optimization_barrier(clip_rows(turned, bound_rows).astype(jnp.bfloat16))
        return (total + coded_rows.astype(jnp.float32), None)
    summed, unused = lax.scan(add_block, jnp.zeros((KV, D), jnp.float32), jnp.arange(BLOCKS, dtype=jnp.int32))
    gradient = unrotate_rows(summed, sign_rows, matrix)
    new_master, new_first, new_second = adam_update(gradient, master_weights, adam_m, adam_v)
    base_full = base_weights.astype(jnp.float32)
    diff_bound = clip_level * jnp.exp2(diff_exps.astype(jnp.float32))
    diff_coded = lax.optimization_barrier(clip_rows(new_master - base_full, diff_bound).astype(jnp.bfloat16))
    effective = (base_full + diff_coded.astype(jnp.float32)).astype(jnp.bfloat16)
    projected = lax.dot_general(tokens, effective, (((1,), (1,)), ((), ())), preferred_element_type=jnp.float32)
    return (projected.astype(jnp.bfloat16), new_master, new_first, new_second)
```

```python
import functools
import math

import jax
import jax.numpy as jnp
import numpy as np
from jax import lax
from jax.experimental import pallas as pl
from jax.experimental.pallas import tpu as pltpu
from jax.sharding import PartitionSpec as P

ADAM_STEP = 10


clip_level = 448.0
beta_one = 0.9
beta_two = 0.95
learn_rate = 0.002
decay_rate = 0.1
adam_eps = 1e-08
highest = lax.Precision.HIGHEST


def hadamard(matrix_size):
    positions = jnp.arange(matrix_size, dtype=jnp.int32)
    common = positions[:, None] & positions[None, :]
    parity = jnp.zeros((matrix_size, matrix_size), jnp.int32)
    for bit_level in range(matrix_size.bit_length() - 1):
        parity = parity + (common >> bit_level & 1)
    return (1 - 2 * (parity % 2)).astype(jnp.float32)


def rotate_rows(row_block, sign_rows, matrix):
    row_count = row_block.shape[0]
    blocks = row_block.reshape(row_count, sign_rows.shape[0], sign_rows.shape[1]) * sign_rows
    turned = jnp.dot(blocks.reshape(-1, sign_rows.shape[1]), matrix, precision=highest)
    return turned.reshape(row_block.shape) / math.sqrt(sign_rows.shape[1])


def unrotate_rows(row_block, sign_rows, matrix):
    row_count = row_block.shape[0]
    turned = jnp.dot(
        row_block.reshape(-1, sign_rows.shape[1]), matrix, precision=highest
    ) / math.sqrt(sign_rows.shape[1])
    return (turned.reshape(row_count, sign_rows.shape[0], sign_rows.shape[1]) * sign_rows).reshape(
        row_block.shape
    )


def clip_rows(row_block, bound_rows):
    row_count = row_block.shape[0]
    shaped = row_block.reshape(row_count, bound_rows.shape[1], -1)
    limits = bound_rows[:, :, None]
    return jnp.clip(shaped, -limits, limits).reshape(row_block.shape)


def adam_update(gradient, master, first, second):
    new_first = beta_one * first + (1.0 - beta_one) * gradient
    new_second = beta_two * second + (1.0 - beta_two) * gradient * gradient
    fix_one = 1.0 - beta_one**ADAM_STEP
    fix_two = 1.0 - beta_two**ADAM_STEP
    step_dir = new_first / fix_one / (jnp.sqrt(new_second / fix_two) + adam_eps)
    new_master = master - learn_rate * (step_dir + decay_rate * master)
    return (new_master, new_first, new_second)


CHUNKS = 16
VMEM_LIMIT = 58000000
DELAYS = (-3, 1, 3, 5, 7, 9, 11, 13, 15, 17, 18)


def z_turn(j):
    return 1 + j % 2


MESH = pl.DeviceIdType.MESH


def step_kernel(
    chunks,
    delays,
    tokens_hbm,
    grad_hbm,
    master_hbm,
    base_hbm,
    first_hbm,
    second_hbm,
    grad_exps_hbm,
    diff_exps_hbm,
    signs_hbm,
    matrix_hbm,
    projected,
    out_master,
    out_first,
    out_second,
    tokens,
    grad_rows,
    master,
    base,
    first,
    second,
    grad_exps,
    diff_exps,
    sign_bits,
    matrix,
    bounds,
    diff_bounds,
    signs,
    grad_t,
    coded,
    rec0,
    sum0,
    rec1,
    sum1,
    rec2,
    sum2,
    rec3,
    sum3,
    rec4,
    gath,
    effective,
    total,
    load_sem,
    send_sem,
    recv_sem,
):
    outer, inner = lax.axis_index("outer"), lax.axis_index("inner")
    xs = 2
    y, c = outer // 2, outer % 2
    z, x = inner // xs, inner % xs
    zh, zl = z // 2, z % 2
    rows = master.shape[0]
    half = grad_t.shape[1]
    width = tokens.shape[1] // chunks
    block_len = sign_bits.shape[1]
    blocks = width // block_len
    groups = half // block_len
    scale = 1.0 / math.sqrt(block_len)
    ahead = 1 - delays[0]
    core_peer = (y * 2 + 1 - c, inner)
    x_peer = (outer, z * xs + 1 - x)
    y_peer = ((1 - y) * 2 + c, inner)
    near_peer = (outer, (zh * 2 + 1 - zl) * xs + x)
    far_peer = (outer, ((1 - zh) * 2 + zl) * xs + x)

    def turns(j, h, along_x, along_y, along_z):
        turn = z_turn(j)
        on0 = (2 - turn) * (1 - turn) // 2
        on1 = turn * (2 - turn)
        on2 = turn * (turn - 1) // 2
        lead = along_x * (1 - h) + along_y * h
        trail = along_y * (1 - h) + along_x * h
        return (
            along_z * on0 + lead * (1 - on0),
            along_z * on1 + lead * on0 + trail * on2,
            along_z * on2 + trail * (1 - on2),
        )

    def mine(j):
        return turns(j, c, x, y, zl) + (zh,)

    def peer_of(j, at):
        if at == 3:
            return far_peer
        return tuple(
            turns(j, c, *ids)[at] for ids in zip(x_peer, y_peer, near_peer)
        )

    barrier = pltpu.get_barrier_semaphore()
    peers = [core_peer, x_peer, y_peer, near_peer, far_peer]
    for peer in peers:
        pl.semaphore_signal(barrier, inc=1, device_id=peer, device_id_type=MESH)

    def load(src, dst, at):
        return pltpu.make_async_copy(src, dst, load_sem.at[at])

    head = pl.ds(0, width)
    tail = pl.ds(width, tokens.shape[1] - width)
    load_grad = load(grad_hbm, grad_rows, 0)
    load_signs = load(signs_hbm, sign_bits, 1)
    load_matrix = load(matrix_hbm, matrix, 2)
    load_head = load(tokens_hbm.at[:, head], tokens.at[:, head], 3)
    load_grad_exps = load(grad_exps_hbm, grad_exps, 4)
    load_tail = load(tokens_hbm.at[:, tail], tokens.at[:, tail], 5)
    late = [
        load(diff_exps_hbm, diff_exps, 6),
        load(master_hbm, master, 7),
        load(first_hbm, first, 8),
        load(second_hbm, second, 9),
        load(base_hbm, base, 10),
    ]
    for item in [load_grad, load_signs, load_matrix, load_head, load_grad_exps, load_tail] + late:
        item.start()

    load_grad.wait()
    for h in range(2):
        for yy in range(2):
            low = (yy * 2 + h) * (half // 2)
            grad_t[h, yy * (half // 2) : (yy + 1) * (half // 2), :] = grad_rows[
                :, low : low + half // 2
            ].T
    load_signs.wait()
    load_matrix.wait()
    load_grad_exps.wait()
    limits = clip_level * jnp.exp2(grad_exps[...].astype(jnp.float32))
    for b in range(sign_bits.shape[0]):
        at = slice(b * block_len, (b + 1) * block_len)
        signs[:, at] = (2 * sign_bits[b : b + 1, :] - 1).astype(jnp.float32)
        bounds[:, at] = jnp.broadcast_to(
            limits[:, b : b + 1], (limits.shape[0], block_len)
        )
    load_head.wait()

    def remote(src, dst, stage, j, peer):
        return pltpu.make_async_remote_copy(
            src_ref=src,
            dst_ref=dst,
            send_sem=send_sem.at[stage, j],
            recv_sem=recv_sem.at[stage, j],
            device_id=peer,
            device_id_type=MESH,
        )

    def copy0(j):
        return remote(coded.at[j, 1 - c], rec0.at[j], 0, j, core_peer)

    def copy1(j):
        return remote(sum0.at[j, 1 - mine(j)[0]], rec1.at[j], 1, j, peer_of(j, 0))

    def copy2(j):
        return remote(sum1.at[j, 1 - mine(j)[1]], rec2.at[j], 2, j, peer_of(j, 1))

    def copy3(j):
        return remote(sum2.at[j, 1 - mine(j)[2]], rec3.at[j], 3, j, peer_of(j, 2))

    def copy4(j):
        return remote(sum3.at[j, 1 - mine(j)[3]], rec4.at[j], 4, j, peer_of(j, 3))

    def gather4(j):
        m = mine(j)
        block = gath.at[j, c, m[0], m[1], m[2], m[3]]
        return remote(block, block, 5, j, peer_of(j, 3))

    def gather3(j):
        m = mine(j)
        block = gath.at[j, c, m[0], m[1], m[2]]
        return remote(block, block, 6, j, peer_of(j, 2))

    def gather2(j):
        m = mine(j)
        block = gath.at[j, c, m[0], m[1]]
        return remote(block, block, 7, j, peer_of(j, 1))

    def gather1(j):
        block = gath.at[j, c, mine(j)[0]]
        return remote(block, block, 8, j, peer_of(j, 0))

    def gather0(j):
        block = gath.at[j, c]
        return remote(block, block, 9, j, core_peer)

    def columns(j):
        return pl.ds(pl.multiple_of(j * width, width), width)

    def produce(j, send=True):
        rotated = jnp.dot(
            tokens[:, columns(j)] * signs[:, columns(j)].astype(jnp.bfloat16),
            matrix[...],
            preferred_element_type=jnp.float32,
        )
        rotated = (rotated * scale).astype(jnp.bfloat16)
        for h in (1 - c, c):
            part = jnp.dot(grad_t[h], rotated, preferred_element_type=jnp.float32)
            for g in range(groups):
                yy, hh = g // 2, g % 2
                limit = bounds[pl.ds(yy * 4 + h * 2 + hh, 1), columns(j)]
                piece = part[g * block_len : (g + 1) * block_len, :]
                piece = jnp.minimum(jnp.maximum(piece, -limit), limit).astype(jnp.bfloat16)
                coded[j, h, yy, hh] = piece.reshape(2, xs, rows, width)
            if send and h is not c:
                copy0(j).start()

    def reduce0(j):
        copy0(j).wait()
        for yy in range(2):
            for hh in range(2):
                for ll in range(2):
                    for xx in range(xs):
                        to1, to2, to3 = turns(j, c, xx, yy, ll)
                        sum0[j, to1, to2, to3, hh] = (
                            coded[j, c, yy, hh, ll, xx] + rec0[j, yy, hh, ll, xx]
                        )
        copy1(j).start()

    def reduce1(j):
        copy1(j).wait()
        sum1[j] = sum0[j, mine(j)[0]] + rec1[j]
        copy2(j).start()

    def reduce2(j):
        copy2(j).wait()
        sum2[j] = sum1[j, mine(j)[1]] + rec2[j]
        copy3(j).start()

    def reduce3(j):
        copy3(j).wait()
        sum3[j] = sum2[j, mine(j)[2]] + rec3[j]
        copy4(j).start()

    def update(j):
        copy4(j).wait()
        summed = sum3[j, zh].astype(jnp.float32) + rec4[j].astype(jnp.float32)
        high = summed.astype(jnp.bfloat16)
        rest = summed - high.astype(jnp.float32)
        middle = rest.astype(jnp.bfloat16)
        low = (rest - middle.astype(jnp.float32)).astype(jnp.bfloat16)
        turned = jnp.dot(
            jnp.concatenate([high, middle, low], axis=0),
            matrix[...],
            preferred_element_type=jnp.float32,
        )
        gradient = (turned[:rows] + turned[rows : 2 * rows]) + turned[2 * rows :]
        gradient = gradient * scale * signs[:, columns(j)]
        own = pl.ds(pl.multiple_of((outer * 8 + inner) * rows, rows), rows)
        new_master, new_first, new_second = adam_update(
            gradient, master[:, columns(j)], first[:, columns(j)], second[:, columns(j)]
        )
        out_master[:, columns(j)] = new_master
        out_first[:, columns(j)] = new_first
        out_second[:, columns(j)] = new_second
        limit = diff_bounds[:, columns(j)]
        change = new_master - base[own, columns(j)].astype(jnp.float32)
        change = jnp.minimum(jnp.maximum(change, -limit), limit)
        m = mine(j)
        gath[j, c, m[0], m[1], m[2], m[3]] = change.astype(jnp.bfloat16)
        gather4(j).start()

    def pass3(j):
        gather4(j).wait()
        gather3(j).start()

    def pass2(j):
        gather3(j).wait()
        gather2(j).start()

    def pass1(j):
        gather2(j).wait()
        gather1(j).start()

    def consume(j, h):
        for yy in range(2):
            for hh in range(2):
                for ll in range(2):
                    for xx in range(xs):
                        at1, at2, at3 = turns(j, h, xx, yy, ll)
                        low = ((yy * 4 + h * 2 + hh) * 4 + ll * 2 + xx) * rows
                        spot = ((yy * 2 + hh) * 4 + ll * 2 + xx) * rows
                        effective[spot : spot + rows, :] = (
                            base[pl.ds(pl.multiple_of(low, rows), rows), columns(j)]
                            + gath[j, h, at1, at2, at3, hh]
                        )
        total[h] += lax.dot_general(
            tokens[:, columns(j)],
            effective[...],
            (((1,), (1,)), ((), ())),
            preferred_element_type=jnp.float32,
        )

    def pass0(j):
        gather1(j).wait()
        gather0(j).start()
        consume(j, c)

    def last(j):
        gather0(j).wait()
        consume(j, 1 - c)

    stages = (
        produce,
        reduce0,
        reduce1,
        reduce2,
        reduce3,
        update,
        pass3,
        pass2,
        pass1,
        pass0,
        last,
    )
    order = (1, 2, 3, 4, 5, 6, 7, 8, 9, 0, 10)

    def step(t, carry):
        for at in order:
            j = t - delays[at]

            @pl.when((j >= 0) & (j < chunks))
            def _():
                stages[at](j)

        return carry

    load_tail.wait()

    def early(j, carry):
        produce(j, send=False)
        return carry

    lax.fori_loop(0, ahead, early, 0)
    pl.semaphore_wait(barrier, len(peers))

    def sent(j, carry):
        copy0(j).start()
        return carry

    lax.fori_loop(0, ahead, sent, 0)
    total[...] = jnp.zeros_like(total)
    late[0].wait()
    spans = clip_level * jnp.exp2(diff_exps[...].astype(jnp.float32))
    for b in range(sign_bits.shape[0]):
        at = slice(b * block_len, (b + 1) * block_len)
        diff_bounds[:, at] = jnp.broadcast_to(spans[:, b : b + 1], (rows, block_len))
    start = min(delays[5], 3)
    lax.fori_loop(1, start, step, 0)
    for item in late[1:]:
        item.wait()
    lax.fori_loop(start, chunks + max(delays), step, 0)
    for h in range(2):
        for yy in range(2):
            low = (yy * 2 + h) * (half // 2)
            projected[:, low : low + half // 2] = total[
                h, :, yy * (half // 2) : (yy + 1) * (half // 2)
            ].astype(jnp.bfloat16)


def write_kernel(*refs):
    sources, targets, sems = refs[:4], refs[4:8], refs[8]
    copies = [
        pltpu.make_async_copy(source, target, sems.at[at])
        for at, (source, target) in enumerate(zip(sources, targets))
    ]
    for item in copies:
        item.start()
    for item in copies:
        item.wait()


def fused_step(
    tokens, out_grad, master, base, first, second, grad_exps, diff_exps, sign_bits, matrix
):
    rows, model_width = master.shape
    token_rows, features = out_grad.shape
    matrix_len = matrix.shape[0]
    width = model_width // CHUNKS
    anywhere = pl.BlockSpec(memory_space=pltpu.HBM)
    vmem = pl.BlockSpec(memory_space=pltpu.VMEM)
    half = jnp.bfloat16
    cell = (rows, width)
    flops = 4 * token_rows * model_width * features
    matrix = jnp.asarray(np.kron(np.eye(width // matrix.shape[0]), matrix), half)
    operands = (
        tokens, out_grad, master, base, first, second, grad_exps, diff_exps, sign_bits, matrix
    )
    results = pl.pallas_call(
        functools.partial(step_kernel, CHUNKS, DELAYS),
        out_shape=(
            pltpu.VMEM((token_rows, features), half),
            pltpu.VMEM(master.shape, jnp.float32),
            pltpu.VMEM(master.shape, jnp.float32),
            pltpu.VMEM(master.shape, jnp.float32),
        ),
        in_specs=[anywhere] * len(operands),
        out_specs=(vmem,) * 4,
        scratch_shapes=[pltpu.VMEM(item.shape, item.dtype) for item in operands]
        + [
            pltpu.VMEM((features // matrix_len, model_width), jnp.float32),
            pltpu.VMEM(master.shape, jnp.float32),
            pltpu.VMEM((1, model_width), jnp.float32),
            pltpu.VMEM((2, features // 2, token_rows), half),
            pltpu.VMEM((CHUNKS, 2, 2, 2, 2, 2) + cell, half),
            pltpu.VMEM((CHUNKS, 2, 2, 2, 2) + cell, half),
            pltpu.VMEM((CHUNKS, 2, 2, 2, 2) + cell, half),
            pltpu.VMEM((CHUNKS, 2, 2, 2) + cell, half),
            pltpu.VMEM((CHUNKS, 2, 2, 2) + cell, half),
            pltpu.VMEM((CHUNKS, 2, 2) + cell, half),
            pltpu.VMEM((CHUNKS, 2, 2) + cell, half),
            pltpu.VMEM((CHUNKS, 2) + cell, half),
            pltpu.VMEM((CHUNKS, 2) + cell, half),
            pltpu.VMEM((CHUNKS,) + cell, half),
            pltpu.VMEM((CHUNKS, 2, 2, 2, 2, 2) + cell, half),
            pltpu.VMEM((features // 2, width), half),
            pltpu.VMEM((2, token_rows, features // 2), jnp.float32),
            pltpu.SemaphoreType.DMA((11,)),
            pltpu.SemaphoreType.DMA((10, CHUNKS)),
            pltpu.SemaphoreType.DMA((10, CHUNKS)),
        ],
        compiler_params=pltpu.CompilerParams(
            collective_id=0, has_side_effects=True, vmem_limit_bytes=VMEM_LIMIT
        ),
        cost_estimate=pl.CostEstimate(flops=flops, bytes_accessed=2**25, transcendentals=0),
    )(*operands)
    return pl.pallas_call(
        write_kernel,
        out_shape=tuple(jax.ShapeDtypeStruct(item.shape, item.dtype) for item in results),
        in_specs=[vmem] * 4,
        out_specs=(anywhere,) * 4,
        scratch_shapes=[pltpu.SemaphoreType.DMA((4,))],
    )(*[pltpu.with_memory_space_constraint(item, pltpu.VMEM) for item in results])


def hadamard_constant(matrix_size):
    matrix = np.ones((1, 1), np.float32)
    while matrix.shape[0] < matrix_size:
        matrix = np.block([[matrix, matrix], [matrix, -matrix]])
    return matrix


def fits_kernel(token_rows, rows_dev, block_len, features, model_width):
    return (
        lax.axis_size("outer") == 4
        and lax.axis_size("inner") == 8
        and rows_dev % 16 == 0
        and token_rows % 16 == 0
        and block_len == 4 * rows_dev
        and features == 32 * rows_dev
        and model_width % (CHUNKS * block_len) == 0
        and features * model_width <= 2**22
        and token_rows <= 384
    )


def shards(
    tokens,
    out_grad,
    master_weights,
    base_weights,
    adam_m,
    adam_v,
    grad_exps,
    diff_exps,
    hadamard_signs,
):
    outer_count = lax.axis_size("outer")
    inner_count = lax.axis_size("inner")
    token_rows = tokens.shape[0]
    model_width = tokens.shape[1]
    rows_dev = master_weights.shape[0]
    sign_rows = (2 * hadamard_signs - 1).astype(jnp.float32)
    block_len = sign_rows.shape[1]
    col_blocks = sign_rows.shape[0]
    matrix = hadamard(block_len)
    bound_all = jnp.repeat(
        clip_level * jnp.exp2(grad_exps[0].astype(jnp.float32)), block_len, axis=0
    )
    if fits_kernel(token_rows, rows_dev, block_len, out_grad.shape[1], model_width):
        return fused_step(
            tokens,
            out_grad,
            master_weights,
            base_weights,
            adam_m,
            adam_v,
            grad_exps[0],
            diff_exps,
            hadamard_signs,
            hadamard_constant(block_len),
        )
    grad_grid = out_grad.reshape(token_rows, outer_count, inner_count, rows_dev).transpose(
        0, 2, 1, 3
    )
    bound_grid = bound_all.reshape(outer_count, inner_count, rows_dev, col_blocks).transpose(
        1, 0, 2, 3
    )
    coded_bound_sel = bound_grid.reshape(-1, col_blocks)
    term_rows = lax.dot_general(
        grad_grid.reshape(token_rows, -1),
        tokens,
        (((0,), (0,)), ((), ())),
        preferred_element_type=jnp.float32,
    )
    turned = rotate_rows(term_rows, sign_rows, matrix)
    coded_rows = lax.optimization_barrier(clip_rows(turned, coded_bound_sel).astype(jnp.bfloat16))
    coded_rows = coded_rows.astype(jnp.float32)
    group_sum = lax.psum_scatter(
        coded_rows.reshape(1 * lax.axis_size("inner"), outer_count, rows_dev, model_width).astype(
            jnp.bfloat16
        ),
        "inner",
        scatter_dimension=0,
        tiled=True,
    )
    summed = (
        lax.psum_scatter(group_sum, "outer", scatter_dimension=1, tiled=True)
        .astype(jnp.float32)
        .reshape(rows_dev, model_width)
    )
    gradient = unrotate_rows(summed, sign_rows, matrix)
    new_master, new_first, new_second = adam_update(gradient, master_weights, adam_m, adam_v)
    owner = lax.axis_index("outer") * inner_count + lax.axis_index("inner")
    base_own = lax.dynamic_slice_in_dim(base_weights, owner * rows_dev, rows_dev, 0).astype(
        jnp.float32
    )
    diff_bound = clip_level * jnp.exp2(diff_exps.astype(jnp.float32))
    diff_coded = clip_rows(new_master - base_own, diff_bound).astype(jnp.bfloat16)
    effective = (
        base_weights.astype(jnp.float32)
        + lax.all_gather(diff_coded, ("outer", "inner"), axis=0, tiled=True).astype(jnp.float32)
    ).astype(jnp.bfloat16)
    result = lax.dot_general(
        tokens, effective, (((1,), (1,)), ((), ())), preferred_element_type=jnp.float32
    )
    projected = result.astype(jnp.bfloat16)
    return (projected, new_master, new_first, new_second)


def solution(mesh):
    in_specs = (
        P(("outer", "inner"), None),
        P(("outer", "inner"), None),
        P(("outer", "inner"), None),
        P(),
        P(("outer", "inner"), None),
        P(("outer", "inner"), None),
        P(("outer", "inner"), None, None),
        P(("outer", "inner"), None),
        P(),
    )
    out_specs = (
        P(("outer", "inner"), None),
        P(("outer", "inner"), None),
        P(("outer", "inner"), None),
        P(("outer", "inner"), None),
    )
    return jax.shard_map(shards, mesh=mesh, in_specs=in_specs, out_specs=out_specs, check_vma=False)
```

```python
import functools
import math

import jax
import jax.numpy as jnp
import numpy as np
from jax import lax
from jax.experimental import pallas as pl
from jax.experimental.pallas import tpu as pltpu
from jax.sharding import PartitionSpec as P

ADAM_STEP = 10


clip_level = 448.0
beta_one = 0.9
beta_two = 0.95
learn_rate = 0.002
decay_rate = 0.1
adam_eps = 1e-08
highest = lax.Precision.HIGHEST


def hadamard(matrix_size):
    positions = jnp.arange(matrix_size, dtype=jnp.int32)
    common = positions[:, None] & positions[None, :]
    parity = jnp.zeros((matrix_size, matrix_size), jnp.int32)
    for bit_level in range(matrix_size.bit_length() - 1):
        parity = parity + (common >> bit_level & 1)
    return (1 - 2 * (parity % 2)).astype(jnp.float32)


def rotate_rows(row_block, sign_rows, matrix):
    row_count = row_block.shape[0]
    blocks = row_block.reshape(row_count, sign_rows.shape[0], sign_rows.shape[1]) * sign_rows
    turned = jnp.dot(blocks.reshape(-1, sign_rows.shape[1]), matrix, precision=highest)
    return turned.reshape(row_block.shape) / math.sqrt(sign_rows.shape[1])


def unrotate_rows(row_block, sign_rows, matrix):
    row_count = row_block.shape[0]
    turned = jnp.dot(
        row_block.reshape(-1, sign_rows.shape[1]), matrix, precision=highest
    ) / math.sqrt(sign_rows.shape[1])
    return (turned.reshape(row_count, sign_rows.shape[0], sign_rows.shape[1]) * sign_rows).reshape(
        row_block.shape
    )


def clip_rows(row_block, bound_rows):
    row_count = row_block.shape[0]
    shaped = row_block.reshape(row_count, bound_rows.shape[1], -1)
    limits = bound_rows[:, :, None]
    return jnp.clip(shaped, -limits, limits).reshape(row_block.shape)


def adam_update(gradient, master, first, second):
    new_first = beta_one * first + (1.0 - beta_one) * gradient
    new_second = beta_two * second + (1.0 - beta_two) * gradient * gradient
    fix_one = 1.0 - beta_one**ADAM_STEP
    fix_two = 1.0 - beta_two**ADAM_STEP
    step_dir = new_first / fix_one / (jnp.sqrt(new_second / fix_two) + adam_eps)
    new_master = master - learn_rate * (step_dir + decay_rate * master)
    return (new_master, new_first, new_second)


CHUNKS = 16
PAIR = 2
VMEM_LIMIT = 58000000
DELAYS = (-3, 1, 3, 5, 7, 9, 11, 13, 15, 18, 19)


def z_turn(j):
    return 1 + j % 2


MESH = pl.DeviceIdType.MESH


def step_kernel(
    chunks,
    delays,
    tokens_hbm,
    grad_hbm,
    master_hbm,
    base_hbm,
    first_hbm,
    second_hbm,
    grad_exps_hbm,
    diff_exps_hbm,
    signs_hbm,
    matrix_hbm,
    projected,
    out_master,
    out_first,
    out_second,
    tokens,
    grad_rows,
    master,
    base,
    first,
    second,
    grad_exps,
    diff_exps,
    sign_bits,
    matrix,
    bounds,
    diff_bounds,
    signs,
    grad_t,
    coded,
    rec0,
    sum0,
    rec1,
    sum1,
    rec2,
    sum2,
    rec3,
    sum3,
    rec4,
    gath,
    effective,
    total,
    load_sem,
    send_sem,
    recv_sem,
):
    outer, inner = lax.axis_index("outer"), lax.axis_index("inner")
    xs = 2
    y, c = outer // 2, outer % 2
    z, x = inner // xs, inner % xs
    zh, zl = z // 2, z % 2
    rows = master.shape[0]
    half = grad_t.shape[1]
    width = tokens.shape[1] // chunks
    block_len = sign_bits.shape[1]
    blocks = width // block_len
    groups = half // block_len
    scale = 1.0 / math.sqrt(block_len)
    pair = effective.shape[1] // width
    ahead = 1 - delays[0]
    core_peer = (y * 2 + 1 - c, inner)
    x_peer = (outer, z * xs + 1 - x)
    y_peer = ((1 - y) * 2 + c, inner)
    near_peer = (outer, (zh * 2 + 1 - zl) * xs + x)
    far_peer = (outer, ((1 - zh) * 2 + zl) * xs + x)

    def turns(j, h, along_x, along_y, along_z):
        turn = z_turn(j)
        on0 = (2 - turn) * (1 - turn) // 2
        on1 = turn * (2 - turn)
        on2 = turn * (turn - 1) // 2
        lead = along_x * (1 - h) + along_y * h
        trail = along_y * (1 - h) + along_x * h
        return (
            along_z * on0 + lead * (1 - on0),
            along_z * on1 + lead * on0 + trail * on2,
            along_z * on2 + trail * (1 - on2),
        )

    def mine(j):
        return turns(j, c, x, y, zl) + (zh,)

    def peer_of(j, at):
        if at == 3:
            return far_peer
        return tuple(
            turns(j, c, *ids)[at] for ids in zip(x_peer, y_peer, near_peer)
        )

    barrier = pltpu.get_barrier_semaphore()
    peers = [core_peer, x_peer, y_peer, near_peer, far_peer]
    for peer in peers:
        pl.semaphore_signal(barrier, inc=1, device_id=peer, device_id_type=MESH)

    def load(src, dst, at):
        return pltpu.make_async_copy(src, dst, load_sem.at[at])

    head = pl.ds(0, width)
    tail = pl.ds(width, tokens.shape[1] - width)
    load_grad = load(grad_hbm, grad_rows, 0)
    load_signs = load(signs_hbm, sign_bits, 1)
    load_matrix = load(matrix_hbm, matrix, 2)
    load_head = load(tokens_hbm.at[:, head], tokens.at[:, head], 3)
    load_grad_exps = load(grad_exps_hbm, grad_exps, 4)
    load_tail = load(tokens_hbm.at[:, tail], tokens.at[:, tail], 5)
    late = [
        load(diff_exps_hbm, diff_exps, 6),
        load(master_hbm, master, 7),
        load(first_hbm, first, 8),
        load(second_hbm, second, 9),
        load(base_hbm, base, 10),
    ]
    for item in [load_grad, load_signs, load_matrix, load_head, load_grad_exps, load_tail] + late:
        item.start()

    load_grad.wait()
    for h in range(2):
        for yy in range(2):
            low = (yy * 2 + h) * (half // 2)
            grad_t[h, yy * (half // 2) : (yy + 1) * (half // 2), :] = grad_rows[
                :, low : low + half // 2
            ].T
    load_signs.wait()
    load_matrix.wait()
    load_grad_exps.wait()
    limits = clip_level * jnp.exp2(grad_exps[...].astype(jnp.float32))
    for b in range(sign_bits.shape[0]):
        at = slice(b * block_len, (b + 1) * block_len)
        signs[:, at] = (2 * sign_bits[b : b + 1, :] - 1).astype(jnp.float32)
        bounds[:, at] = jnp.broadcast_to(
            limits[:, b : b + 1], (limits.shape[0], block_len)
        )
    load_head.wait()

    def remote(src, dst, stage, j, peer):
        return pltpu.make_async_remote_copy(
            src_ref=src,
            dst_ref=dst,
            send_sem=send_sem.at[stage, j],
            recv_sem=recv_sem.at[stage, j],
            device_id=peer,
            device_id_type=MESH,
        )

    def copy0(j):
        return remote(coded.at[j, 1 - c], rec0.at[j], 0, j, core_peer)

    def copy1(j):
        return remote(sum0.at[j, 1 - mine(j)[0]], rec1.at[j], 1, j, peer_of(j, 0))

    def copy2(j):
        return remote(sum1.at[j, 1 - mine(j)[1]], rec2.at[j], 2, j, peer_of(j, 1))

    def copy3(j):
        return remote(sum2.at[j, 1 - mine(j)[2]], rec3.at[j], 3, j, peer_of(j, 2))

    def copy4(j):
        return remote(sum3.at[j, 1 - mine(j)[3]], rec4.at[j], 4, j, peer_of(j, 3))

    def gather4(j):
        m = mine(j)
        block = gath.at[j, c, m[0], m[1], m[2], m[3]]
        return remote(block, block, 5, j, peer_of(j, 3))

    def gather3(j):
        m = mine(j)
        block = gath.at[j, c, m[0], m[1], m[2]]
        return remote(block, block, 6, j, peer_of(j, 2))

    def gather2(j):
        m = mine(j)
        block = gath.at[j, c, m[0], m[1]]
        return remote(block, block, 7, j, peer_of(j, 1))

    def gather1(j):
        block = gath.at[j, c, mine(j)[0]]
        return remote(block, block, 8, j, peer_of(j, 0))

    def gather0(j):
        block = gath.at[j, c]
        return remote(block, block, 9, j, core_peer)

    def columns(j):
        return pl.ds(pl.multiple_of(j * width, width), width)

    def produce(j, send=True):
        rotated = jnp.dot(
            tokens[:, columns(j)] * signs[:, columns(j)].astype(jnp.bfloat16),
            matrix[...],
            preferred_element_type=jnp.float32,
        )
        rotated = (rotated * scale).astype(jnp.bfloat16)
        for h in (1 - c, c):
            part = jnp.dot(grad_t[h], rotated, preferred_element_type=jnp.float32)
            for g in range(groups):
                yy, hh = g // 2, g % 2
                limit = bounds[pl.ds(yy * 4 + h * 2 + hh, 1), columns(j)]
                piece = part[g * block_len : (g + 1) * block_len, :]
                piece = jnp.minimum(jnp.maximum(piece, -limit), limit).astype(jnp.bfloat16)
                coded[j, h, yy, hh] = piece.reshape(2, xs, rows, width)
            if send and h is not c:
                copy0(j).start()

    def reduce0(j):
        copy0(j).wait()
        for yy in range(2):
            for hh in range(2):
                for ll in range(2):
                    for xx in range(xs):
                        to1, to2, to3 = turns(j, c, xx, yy, ll)
                        sum0[j, to1, to2, to3, hh] = (
                            coded[j, c, yy, hh, ll, xx] + rec0[j, yy, hh, ll, xx]
                        )
        copy1(j).start()

    def reduce1(j):
        copy1(j).wait()
        sum1[j] = sum0[j, mine(j)[0]] + rec1[j]
        copy2(j).start()

    def reduce2(j):
        copy2(j).wait()
        sum2[j] = sum1[j, mine(j)[1]] + rec2[j]
        copy3(j).start()

    def reduce3(j):
        copy3(j).wait()
        sum3[j] = sum2[j, mine(j)[2]] + rec3[j]
        copy4(j).start()

    def update(j):
        copy4(j).wait()
        summed = sum3[j, zh].astype(jnp.float32) + rec4[j].astype(jnp.float32)
        high = summed.astype(jnp.bfloat16)
        rest = summed - high.astype(jnp.float32)
        middle = rest.astype(jnp.bfloat16)
        low = (rest - middle.astype(jnp.float32)).astype(jnp.bfloat16)
        turned = jnp.dot(
            jnp.concatenate([high, middle, low], axis=0),
            matrix[...],
            preferred_element_type=jnp.float32,
        )
        gradient = (turned[:rows] + turned[rows : 2 * rows]) + turned[2 * rows :]
        gradient = gradient * scale * signs[:, columns(j)]
        own = pl.ds(pl.multiple_of((outer * 8 + inner) * rows, rows), rows)
        new_master, new_first, new_second = adam_update(
            gradient, master[:, columns(j)], first[:, columns(j)], second[:, columns(j)]
        )
        out_master[:, columns(j)] = new_master
        out_first[:, columns(j)] = new_first
        out_second[:, columns(j)] = new_second
        limit = diff_bounds[:, columns(j)]
        change = new_master - base[own, columns(j)].astype(jnp.float32)
        change = jnp.minimum(jnp.maximum(change, -limit), limit)
        m = mine(j)
        gath[j, c, m[0], m[1], m[2], m[3]] = change.astype(jnp.bfloat16)
        gather4(j).start()

    def pass3(j):
        gather4(j).wait()
        gather3(j).start()

    def pass2(j):
        gather3(j).wait()
        gather2(j).start()

    def pass1(j):
        gather2(j).wait()
        gather1(j).start()

    def consume(j, h):
        @pl.when(j % pair == pair - 1)
        def _():
            first_chunk = j - (pair - 1)
            for k in range(pair):
                for yy in range(2):
                    for hh in range(2):
                        for ll in range(2):
                            for xx in range(xs):
                                at1, at2, at3 = turns(first_chunk + k, h, xx, yy, ll)
                                low = ((yy * 4 + h * 2 + hh) * 4 + ll * 2 + xx) * rows
                                spot = ((yy * 2 + hh) * 4 + ll * 2 + xx) * rows
                                effective[spot : spot + rows, k * width : (k + 1) * width] = (
                                    base[
                                        pl.ds(pl.multiple_of(low, rows), rows),
                                        columns(first_chunk + k),
                                    ]
                                    + gath[first_chunk + k, h, at1, at2, at3, hh]
                                )
            span = pl.ds(pl.multiple_of(first_chunk * width, pair * width), pair * width)
            total[h] += lax.dot_general(
                tokens[:, span],
                effective[...],
                (((1,), (1,)), ((), ())),
                preferred_element_type=jnp.float32,
            )

    def pass0(j):
        gather1(j).wait()
        gather0(j).start()
        consume(j, c)

    def last(j):
        gather0(j).wait()
        consume(j, 1 - c)

    stages = (
        produce,
        reduce0,
        reduce1,
        reduce2,
        reduce3,
        update,
        pass3,
        pass2,
        pass1,
        pass0,
        last,
    )
    order = (1, 2, 3, 4, 5, 6, 7, 8, 9, 0, 10)

    def step(t, carry):
        for at in order:
            j = t - delays[at]

            @pl.when((j >= 0) & (j < chunks))
            def _():
                stages[at](j)

        return carry

    load_tail.wait()

    def early(j, carry):
        produce(j, send=False)
        return carry

    lax.fori_loop(0, ahead, early, 0)
    pl.semaphore_wait(barrier, len(peers))

    def sent(j, carry):
        copy0(j).start()
        return carry

    lax.fori_loop(0, ahead, sent, 0)
    total[...] = jnp.zeros_like(total)
    late[0].wait()
    spans = clip_level * jnp.exp2(diff_exps[...].astype(jnp.float32))
    for b in range(sign_bits.shape[0]):
        at = slice(b * block_len, (b + 1) * block_len)
        diff_bounds[:, at] = jnp.broadcast_to(spans[:, b : b + 1], (rows, block_len))
    start = min(delays[5], 3)
    lax.fori_loop(1, start, step, 0)
    for item in late[1:]:
        item.wait()
    lax.fori_loop(start, chunks + max(delays), step, 0)
    for h in range(2):
        for yy in range(2):
            low = (yy * 2 + h) * (half // 2)
            projected[:, low : low + half // 2] = total[
                h, :, yy * (half // 2) : (yy + 1) * (half // 2)
            ].astype(jnp.bfloat16)


def write_kernel(*refs):
    sources, targets, sems = refs[:4], refs[4:8], refs[8]
    copies = [
        pltpu.make_async_copy(source, target, sems.at[at])
        for at, (source, target) in enumerate(zip(sources, targets))
    ]
    for item in copies:
        item.start()
    for item in copies:
        item.wait()


def fused_step(
    tokens, out_grad, master, base, first, second, grad_exps, diff_exps, sign_bits, matrix
):
    rows, model_width = master.shape
    token_rows, features = out_grad.shape
    matrix_len = matrix.shape[0]
    width = model_width // CHUNKS
    pair = PAIR
    anywhere = pl.BlockSpec(memory_space=pltpu.HBM)
    vmem = pl.BlockSpec(memory_space=pltpu.VMEM)
    half = jnp.bfloat16
    cell = (rows, width)
    flops = 4 * token_rows * model_width * features
    matrix = jnp.asarray(np.kron(np.eye(width // matrix.shape[0]), matrix), half)
    operands = (
        tokens, out_grad, master, base, first, second, grad_exps, diff_exps, sign_bits, matrix
    )
    results = pl.pallas_call(
        functools.partial(step_kernel, CHUNKS, DELAYS),
        out_shape=(
            pltpu.VMEM((token_rows, features), half),
            pltpu.VMEM(master.shape, jnp.float32),
            pltpu.VMEM(master.shape, jnp.float32),
            pltpu.VMEM(master.shape, jnp.float32),
        ),
        in_specs=[anywhere] * len(operands),
        out_specs=(vmem,) * 4,
        scratch_shapes=[pltpu.VMEM(item.shape, item.dtype) for item in operands]
        + [
            pltpu.VMEM((features // matrix_len, model_width), jnp.float32),
            pltpu.VMEM(master.shape, jnp.float32),
            pltpu.VMEM((1, model_width), jnp.float32),
            pltpu.VMEM((2, features // 2, token_rows), half),
            pltpu.VMEM((CHUNKS, 2, 2, 2, 2, 2) + cell, half),
            pltpu.VMEM((CHUNKS, 2, 2, 2, 2) + cell, half),
            pltpu.VMEM((CHUNKS, 2, 2, 2, 2) + cell, half),
            pltpu.VMEM((CHUNKS, 2, 2, 2) + cell, half),
            pltpu.VMEM((CHUNKS, 2, 2, 2) + cell, half),
            pltpu.VMEM((CHUNKS, 2, 2) + cell, half),
            pltpu.VMEM((CHUNKS, 2, 2) + cell, half),
            pltpu.VMEM((CHUNKS, 2) + cell, half),
            pltpu.VMEM((CHUNKS, 2) + cell, half),
            pltpu.VMEM((CHUNKS,) + cell, half),
            pltpu.VMEM((CHUNKS, 2, 2, 2, 2, 2) + cell, half),
            pltpu.VMEM((features // 2, pair * width), half),
            pltpu.VMEM((2, token_rows, features // 2), jnp.float32),
            pltpu.SemaphoreType.DMA((11,)),
            pltpu.SemaphoreType.DMA((10, CHUNKS)),
            pltpu.SemaphoreType.DMA((10, CHUNKS)),
        ],
        compiler_params=pltpu.CompilerParams(
            collective_id=0, has_side_effects=True, vmem_limit_bytes=VMEM_LIMIT
        ),
        cost_estimate=pl.CostEstimate(flops=flops, bytes_accessed=2**25, transcendentals=0),
    )(*operands)
    return pl.pallas_call(
        write_kernel,
        out_shape=tuple(jax.ShapeDtypeStruct(item.shape, item.dtype) for item in results),
        in_specs=[vmem] * 4,
        out_specs=(anywhere,) * 4,
        scratch_shapes=[pltpu.SemaphoreType.DMA((4,))],
    )(*[pltpu.with_memory_space_constraint(item, pltpu.VMEM) for item in results])


def hadamard_constant(matrix_size):
    matrix = np.ones((1, 1), np.float32)
    while matrix.shape[0] < matrix_size:
        matrix = np.block([[matrix, matrix], [matrix, -matrix]])
    return matrix


def fits_kernel(token_rows, rows_dev, block_len, features, model_width):
    return (
        lax.axis_size("outer") == 4
        and lax.axis_size("inner") == 8
        and rows_dev % 16 == 0
        and token_rows % 16 == 0
        and block_len == 4 * rows_dev
        and features == 32 * rows_dev
        and model_width % (CHUNKS * block_len) == 0
        and features * model_width <= 2**22
        and token_rows <= 384
    )


def shards(
    tokens,
    out_grad,
    master_weights,
    base_weights,
    adam_m,
    adam_v,
    grad_exps,
    diff_exps,
    hadamard_signs,
):
    outer_count = lax.axis_size("outer")
    inner_count = lax.axis_size("inner")
    token_rows = tokens.shape[0]
    model_width = tokens.shape[1]
    rows_dev = master_weights.shape[0]
    sign_rows = (2 * hadamard_signs - 1).astype(jnp.float32)
    block_len = sign_rows.shape[1]
    col_blocks = sign_rows.shape[0]
    matrix = hadamard(block_len)
    bound_all = jnp.repeat(
        clip_level * jnp.exp2(grad_exps[0].astype(jnp.float32)), block_len, axis=0
    )
    if fits_kernel(token_rows, rows_dev, block_len, out_grad.shape[1], model_width):
        return fused_step(
            tokens,
            out_grad,
            master_weights,
            base_weights,
            adam_m,
            adam_v,
            grad_exps[0],
            diff_exps,
            hadamard_signs,
            hadamard_constant(block_len),
        )
    grad_grid = out_grad.reshape(token_rows, outer_count, inner_count, rows_dev).transpose(
        0, 2, 1, 3
    )
    bound_grid = bound_all.reshape(outer_count, inner_count, rows_dev, col_blocks).transpose(
        1, 0, 2, 3
    )
    coded_bound_sel = bound_grid.reshape(-1, col_blocks)
    term_rows = lax.dot_general(
        grad_grid.reshape(token_rows, -1),
        tokens,
        (((0,), (0,)), ((), ())),
        preferred_element_type=jnp.float32,
    )
    turned = rotate_rows(term_rows, sign_rows, matrix)
    coded_rows = lax.optimization_barrier(clip_rows(turned, coded_bound_sel).astype(jnp.bfloat16))
    coded_rows = coded_rows.astype(jnp.float32)
    group_sum = lax.psum_scatter(
        coded_rows.reshape(1 * lax.axis_size("inner"), outer_count, rows_dev, model_width).astype(
            jnp.bfloat16
        ),
        "inner",
        scatter_dimension=0,
        tiled=True,
    )
    summed = (
        lax.psum_scatter(group_sum, "outer", scatter_dimension=1, tiled=True)
        .astype(jnp.float32)
        .reshape(rows_dev, model_width)
    )
    gradient = unrotate_rows(summed, sign_rows, matrix)
    new_master, new_first, new_second = adam_update(gradient, master_weights, adam_m, adam_v)
    owner = lax.axis_index("outer") * inner_count + lax.axis_index("inner")
    base_own = lax.dynamic_slice_in_dim(base_weights, owner * rows_dev, rows_dev, 0).astype(
        jnp.float32
    )
    diff_bound = clip_level * jnp.exp2(diff_exps.astype(jnp.float32))
    diff_coded = clip_rows(new_master - base_own, diff_bound).astype(jnp.bfloat16)
    effective = (
        base_weights.astype(jnp.float32)
        + lax.all_gather(diff_coded, ("outer", "inner"), axis=0, tiled=True).astype(jnp.float32)
    ).astype(jnp.bfloat16)
    result = lax.dot_general(
        tokens, effective, (((1,), (1,)), ((), ())), preferred_element_type=jnp.float32
    )
    projected = result.astype(jnp.bfloat16)
    return (projected, new_master, new_first, new_second)


def solution(mesh):
    in_specs = (
        P(("outer", "inner"), None),
        P(("outer", "inner"), None),
        P(("outer", "inner"), None),
        P(),
        P(("outer", "inner"), None),
        P(("outer", "inner"), None),
        P(("outer", "inner"), None, None),
        P(("outer", "inner"), None),
        P(),
    )
    out_specs = (
        P(("outer", "inner"), None),
        P(("outer", "inner"), None),
        P(("outer", "inner"), None),
        P(("outer", "inner"), None),
    )
    return jax.shard_map(shards, mesh=mesh, in_specs=in_specs, out_specs=out_specs, check_vma=False)
```

```python
import functools
import math

import jax
import jax.numpy as jnp
import numpy as np
from jax import lax
from jax.experimental import pallas as pl
from jax.experimental.pallas import tpu as pltpu
from jax.sharding import PartitionSpec as P

ADAM_STEP = 10


clip_level = 448.0
beta_one = 0.9
beta_two = 0.95
learn_rate = 0.002
decay_rate = 0.1
adam_eps = 1e-08
highest = lax.Precision.HIGHEST


def hadamard(matrix_size):
    positions = jnp.arange(matrix_size, dtype=jnp.int32)
    common = positions[:, None] & positions[None, :]
    parity = jnp.zeros((matrix_size, matrix_size), jnp.int32)
    for bit_level in range(matrix_size.bit_length() - 1):
        parity = parity + (common >> bit_level & 1)
    return (1 - 2 * (parity % 2)).astype(jnp.float32)


def rotate_rows(row_block, sign_rows, matrix):
    row_count = row_block.shape[0]
    blocks = row_block.reshape(row_count, sign_rows.shape[0], sign_rows.shape[1]) * sign_rows
    turned = jnp.dot(blocks.reshape(-1, sign_rows.shape[1]), matrix, precision=highest)
    return turned.reshape(row_block.shape) / math.sqrt(sign_rows.shape[1])


def unrotate_rows(row_block, sign_rows, matrix):
    row_count = row_block.shape[0]
    turned = jnp.dot(
        row_block.reshape(-1, sign_rows.shape[1]), matrix, precision=highest
    ) / math.sqrt(sign_rows.shape[1])
    return (turned.reshape(row_count, sign_rows.shape[0], sign_rows.shape[1]) * sign_rows).reshape(
        row_block.shape
    )


def clip_rows(row_block, bound_rows):
    row_count = row_block.shape[0]
    shaped = row_block.reshape(row_count, bound_rows.shape[1], -1)
    limits = bound_rows[:, :, None]
    return jnp.clip(shaped, -limits, limits).reshape(row_block.shape)


def adam_update(gradient, master, first, second):
    new_first = beta_one * first + (1.0 - beta_one) * gradient
    new_second = beta_two * second + (1.0 - beta_two) * gradient * gradient
    fix_one = 1.0 - beta_one**ADAM_STEP
    fix_two = 1.0 - beta_two**ADAM_STEP
    step_dir = new_first / fix_one / (jnp.sqrt(new_second / fix_two) + adam_eps)
    new_master = master - learn_rate * (step_dir + decay_rate * master)
    return (new_master, new_first, new_second)


CHUNKS = 16
PAIR = 2
VMEM_LIMIT = 58000000
DELAYS = (-1, 1, 3, 5, 7, 9, 11, 13, 15, 18, 19)


def z_turn(j):
    return 1 + j % 2


MESH = pl.DeviceIdType.MESH


def step_kernel(
    chunks,
    delays,
    tokens_hbm,
    grad_hbm,
    master_hbm,
    base_hbm,
    first_hbm,
    second_hbm,
    grad_exps_hbm,
    diff_exps_hbm,
    signs_hbm,
    matrix_hbm,
    projected,
    out_master,
    out_first,
    out_second,
    tokens,
    grad_rows,
    master,
    base,
    first,
    second,
    grad_exps,
    diff_exps,
    sign_bits,
    matrix,
    bounds,
    diff_bounds,
    signs,
    grad_t,
    coded,
    rec0,
    sum0,
    rec1,
    sum1,
    rec2,
    sum2,
    rec3,
    sum3,
    rec4,
    gath,
    effective,
    total,
    load_sem,
    send_sem,
    recv_sem,
):
    outer, inner = lax.axis_index("outer"), lax.axis_index("inner")
    xs = 2
    y, c = outer // 2, outer % 2
    z, x = inner // xs, inner % xs
    zh, zl = z // 2, z % 2
    rows = master.shape[0]
    half = grad_t.shape[1]
    width = tokens.shape[1] // chunks
    block_len = sign_bits.shape[1]
    blocks = width // block_len
    groups = half // block_len
    scale = 1.0 / math.sqrt(block_len)
    pair = effective.shape[1] // width
    ahead = 1 - delays[0]
    core_peer = (y * 2 + 1 - c, inner)
    x_peer = (outer, z * xs + 1 - x)
    y_peer = ((1 - y) * 2 + c, inner)
    near_peer = (outer, (zh * 2 + 1 - zl) * xs + x)
    far_peer = (outer, ((1 - zh) * 2 + zl) * xs + x)

    def turns(j, h, along_x, along_y, along_z):
        turn = z_turn(j)
        on0 = (2 - turn) * (1 - turn) // 2
        on1 = turn * (2 - turn)
        on2 = turn * (turn - 1) // 2
        lead = along_x * (1 - h) + along_y * h
        trail = along_y * (1 - h) + along_x * h
        return (
            along_z * on0 + lead * (1 - on0),
            along_z * on1 + lead * on0 + trail * on2,
            along_z * on2 + trail * (1 - on2),
        )

    def mine(j):
        return turns(j, c, x, y, zl) + (zh,)

    def peer_of(j, at):
        if at == 3:
            return far_peer
        return tuple(
            turns(j, c, *ids)[at] for ids in zip(x_peer, y_peer, near_peer)
        )

    barrier = pltpu.get_barrier_semaphore()
    peers = [core_peer, x_peer, y_peer, near_peer, far_peer]
    for peer in peers:
        pl.semaphore_signal(barrier, inc=1, device_id=peer, device_id_type=MESH)

    def load(src, dst, at):
        return pltpu.make_async_copy(src, dst, load_sem.at[at])

    head = pl.ds(0, width)
    tail = pl.ds(width, tokens.shape[1] - width)
    load_grad = load(grad_hbm, grad_rows, 0)
    load_signs = load(signs_hbm, sign_bits, 1)
    load_matrix = load(matrix_hbm, matrix, 2)
    load_head = load(tokens_hbm.at[:, head], tokens.at[:, head], 3)
    load_grad_exps = load(grad_exps_hbm, grad_exps, 4)
    load_tail = load(tokens_hbm.at[:, tail], tokens.at[:, tail], 5)
    late = [
        load(diff_exps_hbm, diff_exps, 6),
        load(master_hbm, master, 7),
        load(first_hbm, first, 8),
        load(second_hbm, second, 9),
        load(base_hbm, base, 10),
    ]
    for item in [load_grad, load_signs, load_matrix, load_head, load_grad_exps, load_tail] + late:
        item.start()

    load_grad.wait()
    for h in range(2):
        for yy in range(2):
            low = (yy * 2 + h) * (half // 2)
            grad_t[h, yy * (half // 2) : (yy + 1) * (half // 2), :] = grad_rows[
                :, low : low + half // 2
            ].T
    load_signs.wait()
    load_matrix.wait()
    load_grad_exps.wait()
    limits = clip_level * jnp.exp2(grad_exps[...].astype(jnp.float32))
    for b in range(sign_bits.shape[0]):
        at = slice(b * block_len, (b + 1) * block_len)
        signs[:, at] = (2 * sign_bits[b : b + 1, :] - 1).astype(jnp.float32)
        bounds[:, at] = jnp.broadcast_to(
            limits[:, b : b + 1], (limits.shape[0], block_len)
        )
    load_head.wait()

    def remote(src, dst, stage, j, peer):
        return pltpu.make_async_remote_copy(
            src_ref=src,
            dst_ref=dst,
            send_sem=send_sem.at[stage, j],
            recv_sem=recv_sem.at[stage, j],
            device_id=peer,
            device_id_type=MESH,
        )

    def copy0(j):
        return remote(coded.at[j, 1 - c], rec0.at[j], 0, j, core_peer)

    def copy1(j):
        return remote(sum0.at[j, 1 - mine(j)[0]], rec1.at[j], 1, j, peer_of(j, 0))

    def copy2(j):
        return remote(sum1.at[j, 1 - mine(j)[1]], rec2.at[j], 2, j, peer_of(j, 1))

    def copy3(j):
        return remote(sum2.at[j, 1 - mine(j)[2]], rec3.at[j], 3, j, peer_of(j, 2))

    def copy4(j):
        return remote(sum3.at[j, 1 - mine(j)[3]], rec4.at[j], 4, j, peer_of(j, 3))

    def gather4(j):
        m = mine(j)
        block = gath.at[j, c, m[0], m[1], m[2], m[3]]
        return remote(block, block, 5, j, peer_of(j, 3))

    def gather3(j):
        m = mine(j)
        block = gath.at[j, c, m[0], m[1], m[2]]
        return remote(block, block, 6, j, peer_of(j, 2))

    def gather2(j):
        m = mine(j)
        block = gath.at[j, c, m[0], m[1]]
        return remote(block, block, 7, j, peer_of(j, 1))

    def gather1(j):
        block = gath.at[j, c, mine(j)[0]]
        return remote(block, block, 8, j, peer_of(j, 0))

    def gather0(j):
        block = gath.at[j, c]
        return remote(block, block, 9, j, core_peer)

    def columns(j):
        return pl.ds(pl.multiple_of(j * width, width), width)

    def produce(j, send=True):
        rotated = jnp.dot(
            tokens[:, columns(j)] * signs[:, columns(j)].astype(jnp.bfloat16),
            matrix[...],
            preferred_element_type=jnp.float32,
        )
        rotated = (rotated * scale).astype(jnp.bfloat16)
        for h in (1 - c, c):
            part = jnp.dot(grad_t[h], rotated, preferred_element_type=jnp.float32)
            for g in range(groups):
                yy, hh = g // 2, g % 2
                limit = bounds[pl.ds(yy * 4 + h * 2 + hh, 1), columns(j)]
                piece = part[g * block_len : (g + 1) * block_len, :]
                piece = jnp.minimum(jnp.maximum(piece, -limit), limit).astype(jnp.bfloat16)
                coded[j, h, yy, hh] = piece.reshape(2, xs, rows, width)
            if send and h is not c:
                copy0(j).start()

    def reduce0(j):
        copy0(j).wait()
        for yy in range(2):
            for hh in range(2):
                for ll in range(2):
                    for xx in range(xs):
                        to1, to2, to3 = turns(j, c, xx, yy, ll)
                        sum0[j, to1, to2, to3, hh] = (
                            coded[j, c, yy, hh, ll, xx] + rec0[j, yy, hh, ll, xx]
                        )
        copy1(j).start()

    def reduce1(j):
        copy1(j).wait()
        sum1[j] = sum0[j, mine(j)[0]] + rec1[j]
        copy2(j).start()

    def reduce2(j):
        copy2(j).wait()
        sum2[j] = sum1[j, mine(j)[1]] + rec2[j]
        copy3(j).start()

    def reduce3(j):
        copy3(j).wait()
        sum3[j] = sum2[j, mine(j)[2]] + rec3[j]
        copy4(j).start()

    def update(j):
        copy4(j).wait()
        summed = sum3[j, zh].astype(jnp.float32) + rec4[j].astype(jnp.float32)
        high = summed.astype(jnp.bfloat16)
        rest = summed - high.astype(jnp.float32)
        middle = rest.astype(jnp.bfloat16)
        low = (rest - middle.astype(jnp.float32)).astype(jnp.bfloat16)
        turned = jnp.dot(
            jnp.concatenate([high, middle, low], axis=0),
            matrix[...],
            preferred_element_type=jnp.float32,
        )
        gradient = (turned[:rows] + turned[rows : 2 * rows]) + turned[2 * rows :]
        gradient = gradient * scale * signs[:, columns(j)]
        own = pl.ds(pl.multiple_of((outer * 8 + inner) * rows, rows), rows)
        new_master, new_first, new_second = adam_update(
            gradient, master[:, columns(j)], first[:, columns(j)], second[:, columns(j)]
        )
        out_master[:, columns(j)] = new_master
        out_first[:, columns(j)] = new_first
        out_second[:, columns(j)] = new_second
        limit = diff_bounds[:, columns(j)]
        change = new_master - base[own, columns(j)].astype(jnp.float32)
        change = jnp.minimum(jnp.maximum(change, -limit), limit)
        m = mine(j)
        gath[j, c, m[0], m[1], m[2], m[3]] = change.astype(jnp.bfloat16)
        gather4(j).start()

    def pass3(j):
        gather4(j).wait()
        gather3(j).start()

    def pass2(j):
        gather3(j).wait()
        gather2(j).start()

    def pass1(j):
        gather2(j).wait()
        gather1(j).start()

    def consume(j, h):
        @pl.when(j % pair == pair - 1)
        def _():
            first_chunk = j - (pair - 1)
            for k in range(pair):
                for yy in range(2):
                    for hh in range(2):
                        for ll in range(2):
                            for xx in range(xs):
                                at1, at2, at3 = turns(first_chunk + k, h, xx, yy, ll)
                                low = ((yy * 4 + h * 2 + hh) * 4 + ll * 2 + xx) * rows
                                spot = ((yy * 2 + hh) * 4 + ll * 2 + xx) * rows
                                effective[spot : spot + rows, k * width : (k + 1) * width] = (
                                    base[
                                        pl.ds(pl.multiple_of(low, rows), rows),
                                        columns(first_chunk + k),
                                    ]
                                    + gath[first_chunk + k, h, at1, at2, at3, hh]
                                )
            span = pl.ds(pl.multiple_of(first_chunk * width, pair * width), pair * width)
            total[h] += lax.dot_general(
                tokens[:, span],
                effective[...],
                (((1,), (1,)), ((), ())),
                preferred_element_type=jnp.float32,
            )

    def pass0(j):
        gather1(j).wait()
        gather0(j).start()
        consume(j, c)

    def last(j):
        gather0(j).wait()
        consume(j, 1 - c)

    stages = (
        produce,
        reduce0,
        reduce1,
        reduce2,
        reduce3,
        update,
        pass3,
        pass2,
        pass1,
        pass0,
        last,
    )
    order = (1, 2, 3, 4, 5, 6, 7, 8, 9, 0, 10)

    def step(t, carry):
        for at in order:
            j = t - delays[at]

            @pl.when((j >= 0) & (j < chunks))
            def _():
                stages[at](j)

        return carry

    load_tail.wait()

    def early(j, carry):
        produce(j, send=False)
        return carry

    lax.fori_loop(0, ahead, early, 0)
    pl.semaphore_wait(barrier, len(peers))

    def sent(j, carry):
        copy0(j).start()
        return carry

    lax.fori_loop(0, ahead, sent, 0)
    total[...] = jnp.zeros_like(total)
    late[0].wait()
    spans = clip_level * jnp.exp2(diff_exps[...].astype(jnp.float32))
    for b in range(sign_bits.shape[0]):
        at = slice(b * block_len, (b + 1) * block_len)
        diff_bounds[:, at] = jnp.broadcast_to(spans[:, b : b + 1], (rows, block_len))
    start = min(delays[5], 3)
    lax.fori_loop(1, start, step, 0)
    for item in late[1:]:
        item.wait()
    lax.fori_loop(start, chunks + max(delays), step, 0)
    for h in range(2):
        for yy in range(2):
            low = (yy * 2 + h) * (half // 2)
            projected[:, low : low + half // 2] = total[
                h, :, yy * (half // 2) : (yy + 1) * (half // 2)
            ].astype(jnp.bfloat16)


def write_kernel(*refs):
    sources, targets, sems = refs[:4], refs[4:8], refs[8]
    copies = [
        pltpu.make_async_copy(source, target, sems.at[at])
        for at, (source, target) in enumerate(zip(sources, targets))
    ]
    for item in copies:
        item.start()
    for item in copies:
        item.wait()


def fused_step(
    tokens, out_grad, master, base, first, second, grad_exps, diff_exps, sign_bits, matrix
):
    rows, model_width = master.shape
    token_rows, features = out_grad.shape
    matrix_len = matrix.shape[0]
    width = model_width // CHUNKS
    pair = PAIR
    anywhere = pl.BlockSpec(memory_space=pltpu.HBM)
    vmem = pl.BlockSpec(memory_space=pltpu.VMEM)
    half = jnp.bfloat16
    cell = (rows, width)
    flops = 4 * token_rows * model_width * features
    matrix = jnp.asarray(np.kron(np.eye(width // matrix.shape[0]), matrix), half)
    operands = (
        tokens, out_grad, master, base, first, second, grad_exps, diff_exps, sign_bits, matrix
    )
    results = pl.pallas_call(
        functools.partial(step_kernel, CHUNKS, DELAYS),
        out_shape=(
            pltpu.VMEM((token_rows, features), half),
            pltpu.VMEM(master.shape, jnp.float32),
            pltpu.VMEM(master.shape, jnp.float32),
            pltpu.VMEM(master.shape, jnp.float32),
        ),
        in_specs=[anywhere] * len(operands),
        out_specs=(vmem,) * 4,
        scratch_shapes=[pltpu.VMEM(item.shape, item.dtype) for item in operands]
        + [
            pltpu.VMEM((features // matrix_len, model_width), jnp.float32),
            pltpu.VMEM(master.shape, jnp.float32),
            pltpu.VMEM((1, model_width), jnp.float32),
            pltpu.VMEM((2, features // 2, token_rows), half),
            pltpu.VMEM((CHUNKS, 2, 2, 2, 2, 2) + cell, half),
            pltpu.VMEM((CHUNKS, 2, 2, 2, 2) + cell, half),
            pltpu.VMEM((CHUNKS, 2, 2, 2, 2) + cell, half),
            pltpu.VMEM((CHUNKS, 2, 2, 2) + cell, half),
            pltpu.VMEM((CHUNKS, 2, 2, 2) + cell, half),
            pltpu.VMEM((CHUNKS, 2, 2) + cell, half),
            pltpu.VMEM((CHUNKS, 2, 2) + cell, half),
            pltpu.VMEM((CHUNKS, 2) + cell, half),
            pltpu.VMEM((CHUNKS, 2) + cell, half),
            pltpu.VMEM((CHUNKS,) + cell, half),
            pltpu.VMEM((CHUNKS, 2, 2, 2, 2, 2) + cell, half),
            pltpu.VMEM((features // 2, pair * width), half),
            pltpu.VMEM((2, token_rows, features // 2), jnp.float32),
            pltpu.SemaphoreType.DMA((11,)),
            pltpu.SemaphoreType.DMA((10, CHUNKS)),
            pltpu.SemaphoreType.DMA((10, CHUNKS)),
        ],
        compiler_params=pltpu.CompilerParams(
            collective_id=0, has_side_effects=True, vmem_limit_bytes=VMEM_LIMIT
        ),
        cost_estimate=pl.CostEstimate(flops=flops, bytes_accessed=2**25, transcendentals=0),
    )(*operands)
    return pl.pallas_call(
        write_kernel,
        out_shape=tuple(jax.ShapeDtypeStruct(item.shape, item.dtype) for item in results),
        in_specs=[vmem] * 4,
        out_specs=(anywhere,) * 4,
        scratch_shapes=[pltpu.SemaphoreType.DMA((4,))],
    )(*[pltpu.with_memory_space_constraint(item, pltpu.VMEM) for item in results])


def hadamard_constant(matrix_size):
    matrix = np.ones((1, 1), np.float32)
    while matrix.shape[0] < matrix_size:
        matrix = np.block([[matrix, matrix], [matrix, -matrix]])
    return matrix


def fits_kernel(token_rows, rows_dev, block_len, features, model_width):
    return (
        lax.axis_size("outer") == 4
        and lax.axis_size("inner") == 8
        and rows_dev % 16 == 0
        and token_rows % 16 == 0
        and block_len == 4 * rows_dev
        and features == 32 * rows_dev
        and model_width % (CHUNKS * block_len) == 0
        and features * model_width <= 2**22
        and token_rows <= 384
    )


def shards(
    tokens,
    out_grad,
    master_weights,
    base_weights,
    adam_m,
    adam_v,
    grad_exps,
    diff_exps,
    hadamard_signs,
):
    outer_count = lax.axis_size("outer")
    inner_count = lax.axis_size("inner")
    token_rows = tokens.shape[0]
    model_width = tokens.shape[1]
    rows_dev = master_weights.shape[0]
    sign_rows = (2 * hadamard_signs - 1).astype(jnp.float32)
    block_len = sign_rows.shape[1]
    col_blocks = sign_rows.shape[0]
    matrix = hadamard(block_len)
    bound_all = jnp.repeat(
        clip_level * jnp.exp2(grad_exps[0].astype(jnp.float32)), block_len, axis=0
    )
    if fits_kernel(token_rows, rows_dev, block_len, out_grad.shape[1], model_width):
        return fused_step(
            tokens,
            out_grad,
            master_weights,
            base_weights,
            adam_m,
            adam_v,
            grad_exps[0],
            diff_exps,
            hadamard_signs,
            hadamard_constant(block_len),
        )
    grad_grid = out_grad.reshape(token_rows, outer_count, inner_count, rows_dev).transpose(
        0, 2, 1, 3
    )
    bound_grid = bound_all.reshape(outer_count, inner_count, rows_dev, col_blocks).transpose(
        1, 0, 2, 3
    )
    coded_bound_sel = bound_grid.reshape(-1, col_blocks)
    term_rows = lax.dot_general(
        grad_grid.reshape(token_rows, -1),
        tokens,
        (((0,), (0,)), ((), ())),
        preferred_element_type=jnp.float32,
    )
    turned = rotate_rows(term_rows, sign_rows, matrix)
    coded_rows = lax.optimization_barrier(clip_rows(turned, coded_bound_sel).astype(jnp.bfloat16))
    coded_rows = coded_rows.astype(jnp.float32)
    group_sum = lax.psum_scatter(
        coded_rows.reshape(1 * lax.axis_size("inner"), outer_count, rows_dev, model_width).astype(
            jnp.bfloat16
        ),
        "inner",
        scatter_dimension=0,
        tiled=True,
    )
    summed = (
        lax.psum_scatter(group_sum, "outer", scatter_dimension=1, tiled=True)
        .astype(jnp.float32)
        .reshape(rows_dev, model_width)
    )
    gradient = unrotate_rows(summed, sign_rows, matrix)
    new_master, new_first, new_second = adam_update(gradient, master_weights, adam_m, adam_v)
    owner = lax.axis_index("outer") * inner_count + lax.axis_index("inner")
    base_own = lax.dynamic_slice_in_dim(base_weights, owner * rows_dev, rows_dev, 0).astype(
        jnp.float32
    )
    diff_bound = clip_level * jnp.exp2(diff_exps.astype(jnp.float32))
    diff_coded = clip_rows(new_master - base_own, diff_bound).astype(jnp.bfloat16)
    effective = (
        base_weights.astype(jnp.float32)
        + lax.all_gather(diff_coded, ("outer", "inner"), axis=0, tiled=True).astype(jnp.float32)
    ).astype(jnp.bfloat16)
    result = lax.dot_general(
        tokens, effective, (((1,), (1,)), ((), ())), preferred_element_type=jnp.float32
    )
    projected = result.astype(jnp.bfloat16)
    return (projected, new_master, new_first, new_second)


def solution(mesh):
    in_specs = (
        P(("outer", "inner"), None),
        P(("outer", "inner"), None),
        P(("outer", "inner"), None),
        P(),
        P(("outer", "inner"), None),
        P(("outer", "inner"), None),
        P(("outer", "inner"), None, None),
        P(("outer", "inner"), None),
        P(),
    )
    out_specs = (
        P(("outer", "inner"), None),
        P(("outer", "inner"), None),
        P(("outer", "inner"), None),
        P(("outer", "inner"), None),
    )
    return jax.shard_map(shards, mesh=mesh, in_specs=in_specs, out_specs=out_specs, check_vma=False)
```
